32 devices in a mesh: tile: 16 (over z, y, x), member: 2 (over core).
Axes of the slice: x: 2, y: 2, z: 4, core: 2. Of those that a mesh axis runs over, the one named last changes fastest.
Arguments:
- pixels: bfloat16 [96, 400, 1152], P('tile', 'member'), parts along dimension 1, may hold values from -6 to 6
- channel_index_table: int32 [16, 6], P('tile'), may hold values from 0 to 68, as said below
- group_sizes: int32 [16], P('tile'), may hold values from 0 to 6, as said below
- patch_weight: bfloat16 [9, 200, 512], replicated, may hold values from -0.4375 to 0.4375
- patch_bias: bfloat16 [9, 512], replicated, may hold values from -3 to 3
- level_code: bfloat16 [14, 512], replicated, may hold values from -3 to 3
- latents: bfloat16 [3, 512], replicated
- perc_query: bfloat16 [512, 512], replicated, may hold values from -0.25 to 0.25
- perc_kv: bfloat16 [512, 1024], replicated, may hold values from -0.25 to 0.25
- perc_out: bfloat16 [512, 512], replicated, may hold values from -0.25 to 0.25
- norm_gain: bfloat16 [512], replicated, may hold values from 0.5 to 1.5
- window_qkv: bfloat16 [512, 1536], replicated
- window_out: bfloat16 [512, 512], replicated, may hold values from -0.25 to 0.25
- shift: int32 [1], replicated, may hold values from 1 to 11
Outputs:
- encoded: bfloat16 [4, 16, 12, 12, 512], P(None, 'tile', 'member'), parts along dimension 2
The draws below stay inside these ranges and needn't reach their ends.
There are 2 independent parts, one for each index of `member`. The reference program is written for one: setup_inputs(seed, part) draws one part's arguments, and reference() takes and returns one part's arrays. A program takes and returns all parts, laid end to end along the dimension named above; an argument that names none is the same for every part. Nothing has to cross between parts.
Inputs may be any that keep to these rules, and one draw needn't show every extreme that they name: `channel_index_table`: slots 0 to group_sizes - 1 of the devices hold distinct channels, and together every one of the 69 channels once; channel c < 65 is variable c // 13 at level c % 13, the others are surface variables; other slots hold any channel number. `group_sizes`: they sum to 69; some device holds 6.
All inputs are finite; a program needn't handle non-finite values.
Results may differ from the reference program's by a relative error of at most 0.0095.
Values may be sent and summed in bfloat16 or wider, within the bound.
A program may use at most 128 MiB of HBM per device.

```python
import math
import jax
import jax.numpy as jnp
from jax import lax

E = 512
LEVELS = 13
V_ATM = 5
V_SURF = 4
LATENT = 3
HEADS = 8
WL = 2
WH = 6
WW = 12
LT = 8
TW = 12
PIX = 200
CHANNELS = 69
KINDS = 9
CAP = 6
SLOTS = 96
BANDS = 2
ROWS = 12
LON = 96
NP = 1152
N_TILE = 16


def assign_slots(key):
    base = jax.random.fold_in(key, 11)
    first_key, second_key, third_key, fourth_key = jax.random.split(base, 4)
    total_slots = N_TILE * CAP
    slot_index = jnp.arange(total_slots, dtype=jnp.int32)
    whole_device_input = jax.random.randint(first_key, (), 0, N_TILE)
    attention_logits = jax.random.permutation(second_key, total_slots).astype(jnp.int32) + CAP
    attention_logits = jnp.where(slot_index // CAP == whole_device_input, slot_index % CAP, attention_logits)
    order = jnp.argsort(attention_logits, stable=True).astype(jnp.int32)
    rank_order = jnp.zeros((total_slots,), jnp.int32).at[order].set(slot_index)
    chosen = (rank_order < CHANNELS).astype(jnp.int32)
    sizes = jnp.sum(chosen.reshape(N_TILE, CAP), axis=1).astype(jnp.int32)
    live = slot_index % CAP < sizes[slot_index // CAP]
    position = jnp.clip(jnp.cumsum(live.astype(jnp.int32)) - 1, 0, CHANNELS - 1)
    channel_order = jax.random.permutation(third_key, CHANNELS).astype(jnp.int32)
    filler = jax.random.randint(fourth_key, (total_slots,), 0, CHANNELS)
    slot_ids = jnp.where(live, channel_order[position], filler).astype(jnp.int32)
    return (slot_ids.reshape(N_TILE, CAP), sizes)


def draw_channel_index_table(key, part):
    return assign_slots(key)[0]


def draw_group_sizes(key, part):
    return assign_slots(key)[1]


def draw_latents(key, part):
    first_key = jax.random.fold_in(jax.random.fold_in(key, 23), 0)
    values = jax.random.normal(first_key, (LATENT, E), jnp.float32)
    return values.astype(jnp.bfloat16)


def draw_window_qkv(key, part):
    first_key = jax.random.fold_in(jax.random.fold_in(key, 37), 0)
    values = jax.random.normal(first_key, (E, 3 * E), jnp.float32) / math.sqrt(E)
    return values.astype(jnp.bfloat16)


def levels(stream_key, extent, cuts, low, high):
    level = 1.0
    for axis_at, blocks in cuts:
        heights = jax.random.uniform(jax.random.fold_in(jax.random.fold_in(stream_key, 6), axis_at), (blocks,), jnp.float32, low / len(cuts), high / len(cuts))
        level = level * jnp.repeat(jnp.exp(heights), extent[axis_at] // blocks).reshape((-1,) + (1,) * (len(extent) - 1 - axis_at))
    return level


def normal_values(rng, dims, scale, most, cuts=(), kind=jnp.bfloat16):
    level = levels(rng, dims, cuts, -0.22, 0.18) if cuts else 1.0
    values = jax.random.normal(rng, dims, jnp.float32) * scale * level
    return jnp.minimum(jnp.maximum(values, -most), most).astype(kind)


def setup_inputs(seed: int = 0, part: int = 0) -> dict:
    seeds = jax.random.split(jax.random.key(seed), 15)
    part_splits = jax.random.split(jax.random.fold_in(seeds[14], part), 15)
    return {
        "pixels": normal_values(part_splits[0], (SLOTS, PIX, NP), 1.0, 6.0, ((0, 16),)),
        "channel_index_table": draw_channel_index_table(jax.random.fold_in(seeds[14], 71), part),
        "group_sizes": draw_group_sizes(jax.random.fold_in(seeds[14], 71), part),
        "patch_weight": normal_values(seeds[3], (KINDS, PIX, E), PIX ** -0.5, 0.4375),
        "patch_bias": normal_values(seeds[4], (KINDS, E), 0.5, 3.0),
        "level_code": normal_values(seeds[5], (LEVELS + 1, E), 0.5, 3.0),
        "latents": draw_latents(jax.random.fold_in(seeds[14], 71), part),
        "perc_query": normal_values(seeds[7], (E, E), E ** -0.5, 0.25),
        "perc_kv": normal_values(seeds[8], (E, 2 * E), E ** -0.5, 0.25),
        "perc_out": normal_values(seeds[9], (E, E), E ** -0.5, 0.25),
        "norm_gain": jnp.clip(1.0 + 0.1 * jax.random.normal(seeds[10], (E,), jnp.float32), 0.5, 1.5).astype(jnp.bfloat16),
        "window_qkv": draw_window_qkv(jax.random.fold_in(seeds[14], 71), part),
        "window_out": normal_values(seeds[12], (E, E), E ** -0.5, 0.25),
        "shift": jax.random.randint(seeds[13], (1,), 1, WW).astype(jnp.int32),
    }


def layer_norm(values, norm_gain):
    center = values - lax.optimization_barrier(jnp.mean(values, axis=-1, keepdims=True))
    spread = lax.optimization_barrier(jnp.mean(center * center, axis=-1, keepdims=True))
    return center * lax.rsqrt(spread + 1e-05) * norm_gain.astype(jnp.float32)

def embed_channels(chosen, kinds, raw_channels, patch_weight, patch_bias):
    inputs = raw_channels[chosen].astype(jnp.float32)
    attention_weight = patch_weight[kinds].astype(jnp.float32)
    result = jnp.einsum('ckp,cke->cpe', inputs, attention_weight)
    return (result + patch_bias[kinds].astype(jnp.float32)[:, None, :]).astype(jnp.bfloat16)

def reference(pixels, channel_index_table, group_sizes, patch_weight, patch_bias, level_code, latents, perc_query, perc_kv, perc_out, norm_gain, window_qkv, window_out, shift):
    width = E
    head_size = width // HEADS
    slot_index = jnp.arange(SLOTS, dtype=jnp.int32)
    live = slot_index % CAP < group_sizes[slot_index // CAP]
    flat_ids = channel_index_table.reshape(-1)
    match_table = ((flat_ids[None, :] == jnp.arange(CHANNELS, dtype=jnp.int32)[:, None]) & live[None, :]).astype(jnp.int32)
    slot_of = jnp.argmax(match_table, axis=1).astype(jnp.int32)
    raw_channels = pixels[slot_of]
    level_sum = jnp.zeros((LEVELS, NP, width), jnp.float32)
    for variable in range(V_ATM):
        chosen = jnp.arange(LEVELS, dtype=jnp.int32) + variable * LEVELS
        kinds = jnp.full((LEVELS,), variable, jnp.int32)
        level_sum = level_sum + embed_channels(chosen, kinds, raw_channels, patch_weight, patch_bias).astype(jnp.float32)
    chosen = jnp.arange(V_SURF, dtype=jnp.int32) + V_ATM * LEVELS
    kinds = jnp.arange(V_SURF, dtype=jnp.int32) + V_ATM
    surface_sum = lax.optimization_barrier(jnp.sum(embed_channels(chosen, kinds, raw_channels, patch_weight, patch_bias).astype(jnp.float32), axis=0))
    codes = level_code.astype(jnp.float32)
    level_tokens = (level_sum + codes[:LEVELS, None, :]).astype(jnp.bfloat16)
    surface = surface_sum + codes[LEVELS]
    pair = jnp.dot(level_tokens.reshape(-1, width), perc_kv, preferred_element_type=jnp.float32).astype(jnp.bfloat16)
    pair = pair.reshape(LEVELS, NP, 2, HEADS, head_size).astype(jnp.float32)
    query = jnp.dot(latents, perc_query, preferred_element_type=jnp.float32).reshape(LATENT, HEADS, head_size)
    attention_logits = jnp.einsum('jhd,lphd->jphl', query, pair[:, :, 0]) / math.sqrt(head_size)
    attn_b = jax.nn.softmax(attention_logits, axis=-1).astype(jnp.bfloat16).astype(jnp.float32)
    gathered = jnp.einsum('jphl,lphd->jphd', attn_b, pair[:, :, 1]).astype(jnp.bfloat16).reshape(LATENT * NP, width)
    latent_state = latents.astype(jnp.float32)[:, None, :] + jnp.dot(gathered, perc_out, preferred_element_type=jnp.float32).reshape(LATENT, NP, width)
    state = jnp.concatenate([latent_state, surface[None]], axis=0)
    grid = state.reshape(LATENT + 1, LT, BANDS, WH, TW, width).transpose(0, 2, 3, 1, 4, 5).reshape(LATENT + 1, ROWS, LON, width)
    normed = layer_norm(grid, norm_gain).astype(jnp.bfloat16)
    offset = shift[0]
    rolled = jnp.roll(normed, -offset, axis=2)
    count_columns = LON // WW
    level_groups = (LATENT + 1) // WL
    triple = jnp.dot(rolled.reshape(-1, width), window_qkv, preferred_element_type=jnp.float32).astype(jnp.bfloat16)
    triple = triple.reshape(level_groups, WL, BANDS, WH, count_columns, WW, 3, HEADS, head_size).transpose(0, 2, 4, 1, 3, 5, 6, 7, 8)
    triple = triple.reshape(level_groups * BANDS * count_columns, WL * WH * WW, 3, HEADS, head_size).astype(jnp.float32)

    def single_window(packed):
        logits = jnp.einsum('qhd,khd->hqk', packed[:, 0], packed[:, 1]) / math.sqrt(head_size)
        attention_weight = jax.nn.softmax(logits, axis=-1).astype(jnp.bfloat16).astype(jnp.float32)
        return jnp.einsum('hqk,khd->qhd', attention_weight, packed[:, 2]).astype(jnp.bfloat16)
    mixed = lax.map(single_window, triple)
    mixed = mixed.reshape(level_groups, BANDS, count_columns, WL, WH, WW, width).transpose(0, 3, 1, 4, 2, 5, 6).reshape(LATENT + 1, ROWS, LON, width)
    projected = jnp.dot(mixed.reshape(-1, width), window_out, preferred_element_type=jnp.float32).reshape(LATENT + 1, ROWS, LON, width)
    projected = jnp.roll(projected, offset, axis=2)
    result = (grid + projected).astype(jnp.bfloat16)
    result = result.reshape(LATENT + 1, BANDS, WH, LT, TW, width).transpose(0, 3, 1, 2, 4, 5)
    return result.reshape(LATENT + 1, N_TILE, WH, TW, width)
```

```python
import functools
import math

import jax
import jax.numpy as jnp
from jax import lax
from jax.experimental import pallas as pl
from jax.experimental.pallas import tpu as pltpu
from jax.sharding import PartitionSpec as P

LEVELS = 13
V_ATM = 5
V_SURF = 4
LATENT = 3
HEADS = 8
WL = 2
WH = 6
WW = 12
LT = 8
CHANNELS = V_ATM * LEVELS + V_SURF
F32 = jnp.float32
BF16 = jnp.bfloat16
NT = (((1,), (1,)), ((), ()))


def exchange_and_perceive(
    n, cap, kinds, slot_of, x_ref, weight, bias, code, latents, perc_query, perc_kv,
    perc_out, gain, state_ref, normed_ref, recv, emb, pair, logits, gath, send_sem, recv_sem,
):
    me = lax.axis_index("tile")
    member = lax.axis_index("member")
    patches, packed = x_ref.shape[1:]
    pix = packed // cap
    width = weight.shape[2]
    head = width // HEADS

    barrier = pltpu.get_barrier_semaphore()

    def greet(k, carry):
        pl.semaphore_signal(barrier, inc=1, device_id={"tile": lax.rem(me + k, n)})
        return carry

    lax.fori_loop(1, n, greet, 0)
    pl.semaphore_wait(barrier, n - 1)

    def offset(i):
        half = n // 2
        step = (i + 1) // 2
        return half + step - 2 * step * (i % 2)

    def copy(k):
        to = lax.rem(me + k, n)
        return pltpu.make_async_remote_copy(
            src_ref=x_ref.at[to],
            dst_ref=recv.at[me],
            send_sem=send_sem.at[k],
            recv_sem=recv_sem.at[k],
            device_id={"tile": to},
        )

    def launch(i, carry):
        copy(offset(i)).start()
        return carry

    lax.fori_loop(0, n - 1, launch, 0)

    def embed(block, source):
        for s in range(cap):
            slot = source * cap + s
            kind = kinds[slot]
            value = jnp.dot(
                block[:, s * pix:(s + 1) * pix], weight[kind], preferred_element_type=F32
            )
            emb[slot] = (value + bias[kind].astype(F32)).astype(BF16)

    embed(x_ref[me], me)

    query = jnp.dot(latents[...], perc_query[...], preferred_element_type=F32) / math.sqrt(head)
    lane_head = lax.broadcasted_iota(jnp.int32, (HEADS, width), 1) // head
    row_head = lax.broadcasted_iota(jnp.int32, (HEADS, width), 0)
    own_head = lane_head == row_head
    spread = [jnp.where(own_head, query[j:j + 1, :], 0.0) for j in range(LATENT)]
    spread.append(jnp.zeros((HEADS, width), F32))
    rows = jnp.concatenate(spread, axis=0)
    rows_high = rows.astype(BF16)
    rows_low = (rows - rows_high.astype(F32)).astype(BF16)

    def land(i, carry):
        k = offset(i)
        copy(k).wait_recv()
        source = lax.rem(me + n - k, n)
        embed(recv[source], source)
        return carry

    lax.fori_loop(0, n - 1, land, 0)

    def one_level(l, carry):
        total = emb[slot_of[l]].astype(F32)
        for v in range(1, V_ATM):
            total = total + emb[slot_of[v * LEVELS + l]].astype(F32)
        token = (total + code[l].astype(F32)).astype(BF16)
        both = jnp.dot(token, perc_kv[...], preferred_element_type=F32).astype(BF16)
        pair[l] = both[:, width:]
        keys = both[:, :width]
        logits[l] = lax.dot_general(
            keys, rows_high, NT, preferred_element_type=F32
        ) + lax.dot_general(keys, rows_low, NT, preferred_element_type=F32)
        return carry

    lax.fori_loop(0, LEVELS, one_level, 0)

    top = logits[0]
    for l in range(1, LEVELS):
        top = jnp.maximum(top, logits[l])
    norm = jnp.zeros_like(top)
    for l in range(LEVELS):
        power = jnp.exp(logits[l] - top)
        logits[l] = power
        norm = norm + power
    scale = 1.0 / norm

    wide_row = lax.broadcasted_iota(jnp.int32, (4 * HEADS, LATENT * width), 0)
    wide_lane = lax.broadcasted_iota(jnp.int32, (4 * HEADS, LATENT * width), 1) // head
    expand = jnp.where(wide_row == wide_lane, 1.0, 0.0).astype(BF16)
    gath[...] = jnp.zeros_like(gath)

    def weigh(l, carry):
        attn = (logits[l] * scale).astype(BF16)
        value = pair[l].astype(F32)
        wide = jnp.dot(attn, expand, preferred_element_type=F32)
        for j in range(LATENT):
            gath[j] += wide[:, j * width:(j + 1) * width] * value
        return carry

    lax.fori_loop(0, LEVELS, weigh, 0)

    surface = emb[slot_of[V_ATM * LEVELS]].astype(F32)
    for c in range(V_ATM * LEVELS + 1, CHANNELS):
        surface = surface + emb[slot_of[c]].astype(F32)
    surface = surface + code[LEVELS].astype(F32)
    for j in range(LATENT + 1):
        if j < LATENT:
            state = latents[j:j + 1, :].astype(F32) + jnp.dot(
                gath[j].astype(BF16), perc_out[...], preferred_element_type=F32
            )
        else:
            state = surface
        center = state - jnp.mean(state, axis=-1, keepdims=True)
        spread_of = jnp.mean(center * center, axis=-1, keepdims=True)
        state_ref[j] = state
        normed_ref[j] = (
            center * lax.rsqrt(spread_of + 1e-05) * gain[...].astype(F32)
        ).astype(BF16)

    def drain(i, carry):
        copy(offset(i)).wait_send()
        return carry

    lax.fori_loop(0, n - 1, drain, 0)


def window_attention(
    shift_ref, state_ref, own_ref, left_ref, right_ref, qkv_ref, out_w_ref, out_ref,
    own_triple, near_pair, mixed_ref,
):
    levels, patches, width = own_ref.shape
    head = width // HEADS
    members = WL * patches
    offset = shift_ref[0]
    rows = levels * patches
    column = lax.broadcasted_iota(jnp.int32, (levels, patches, width), 1) % WW
    near = jnp.where(
        column >= offset, left_ref[...].astype(F32), right_ref[...].astype(F32)
    ).astype(BF16)
    own_triple[...] = jnp.dot(
        own_ref[...].reshape(rows, width), qkv_ref[...], preferred_element_type=F32
    ).astype(BF16)
    near_pair[...] = jnp.dot(
        near.reshape(rows, width), qkv_ref[:, width:], preferred_element_type=F32
    ).astype(BF16)
    q_first = lax.broadcasted_iota(jnp.int32, (members, members), 0) % WW < offset
    k_first = lax.broadcasted_iota(jnp.int32, (members, members), 1) % WW < offset
    same = q_first == k_first
    lane = lax.broadcasted_iota(jnp.int32, (members, 2 * head), 1) // head
    scale = 1.0 / math.sqrt(head)
    for g in range(levels // WL):
        r = slice(g * members, (g + 1) * members)
        for h2 in range(HEADS // 2):
            c = slice(h2 * 2 * head, (h2 + 1) * 2 * head)
            ck = slice(width + h2 * 2 * head, width + (h2 + 1) * 2 * head)
            cv = slice(2 * width + h2 * 2 * head, 2 * width + (h2 + 1) * 2 * head)
            q = own_triple[r, c]
            k_own = own_triple[r, ck]
            v_own = own_triple[r, cv]
            k_near = near_pair[r, c]
            v_near = near_pair[r, ck]
            halves = []
            for one in range(2):
                q_one = jnp.where(lane == one, q, jnp.zeros_like(q))
                a = lax.dot_general(q_one, k_own, NT, preferred_element_type=F32) * scale
                b = lax.dot_general(q_one, k_near, NT, preferred_element_type=F32) * scale
                a = jnp.where(same, a, -jnp.inf)
                b = jnp.where(same, -jnp.inf, b)
                top = jnp.maximum(
                    jnp.max(a, axis=-1, keepdims=True), jnp.max(b, axis=-1, keepdims=True)
                )
                a = jnp.exp(a - top)
                b = jnp.exp(b - top)
                norm = 1.0 / (
                    jnp.sum(a, axis=-1, keepdims=True) + jnp.sum(b, axis=-1, keepdims=True)
                )
                halves.append(
                    jnp.dot((a * norm).astype(BF16), v_own, preferred_element_type=F32)
                    + jnp.dot((b * norm).astype(BF16), v_near, preferred_element_type=F32)
                )
            mixed_ref[r, c] = jnp.where(lane == 0, halves[0], halves[1]).astype(BF16)
    result = state_ref[...].reshape(rows, width) + jnp.dot(
        mixed_ref[...], out_w_ref[...], preferred_element_type=F32
    )
    for i in range(levels * WH):
        out_ref[i // WH, 0, i % WH] = result[i * WW:(i + 1) * WW, :].astype(BF16)


def passed_along(block, axis, distance):
    devices = range(lax.axis_size(axis))
    route = [((i - distance) % len(devices), i) for i in devices]
    return lax.ppermute(block, axis, route)


def local(
    pixels, channel_index_table, group_sizes, patch_weight, patch_bias, level_code, latents,
    perc_query, perc_kv, perc_out, norm_gain, window_qkv, window_out, shift,
):
    n = lax.axis_size("tile")
    bands = n // LT
    cap, pix, all_patches = pixels.shape
    patches = all_patches // n
    kind_count, _, width = patch_weight.shape
    vmem = pl.BlockSpec(memory_space=pltpu.VMEM)
    smem = pl.BlockSpec(memory_space=pltpu.SMEM)

    slot = jnp.arange(cap, dtype=jnp.int32)[None, :]
    marked = jnp.where(
        slot < group_sizes[:, None], channel_index_table, channel_index_table + CHANNELS
    )
    marked = lax.all_gather(marked, "tile", axis=0, tiled=True).reshape(-1)
    slot_of = jnp.argmax(
        marked[None, :] == jnp.arange(CHANNELS, dtype=jnp.int32)[:, None], axis=1
    ).astype(jnp.int32)
    ids = marked % CHANNELS
    kinds = jnp.where(ids < V_ATM * LEVELS, ids // LEVELS, ids - V_ATM * LEVELS + V_ATM)

    blocks = pixels.reshape(cap * pix, all_patches).T.reshape(n, patches, cap * pix)
    state, normed = pl.pallas_call(
        functools.partial(exchange_and_perceive, n, cap),
        out_shape=(
            jax.ShapeDtypeStruct((LATENT + 1, patches, width), F32),
            jax.ShapeDtypeStruct((LATENT + 1, patches, width), BF16),
        ),
        in_specs=[smem, smem] + [vmem] * 9,
        out_specs=(vmem, vmem),
        scratch_shapes=[
            pltpu.VMEM((n, patches, cap * pix), BF16),
            pltpu.VMEM((n * cap, patches, width), BF16),
            pltpu.VMEM((LEVELS, patches, width), BF16),
            pltpu.VMEM((LEVELS, patches, 4 * HEADS), F32),
            pltpu.VMEM((LATENT, patches, width), F32),
            pltpu.SemaphoreType.DMA((n,)),
            pltpu.SemaphoreType.DMA((n,)),
        ],
        compiler_params=pltpu.CompilerParams(
            collective_id=0, has_side_effects=True, vmem_limit_bytes=60 * 1024 * 1024
        ),
    )(
        kinds, slot_of, blocks, patch_weight, patch_bias.reshape(kind_count, 1, width),
        level_code.reshape(LEVELS + 1, 1, width), latents, perc_query, perc_kv, perc_out,
        norm_gain.reshape(1, width),
    )
    left = passed_along(normed, "tile", bands)
    right = passed_along(normed, "tile", -bands)
    return pl.pallas_call(
        window_attention,
        out_shape=jax.ShapeDtypeStruct((LATENT + 1, 1, WH, patches // WH, width), BF16),
        in_specs=[smem] + [vmem] * 6,
        out_specs=vmem,
        scratch_shapes=[
            pltpu.VMEM(((LATENT + 1) * patches, 3 * width), BF16),
            pltpu.VMEM(((LATENT + 1) * patches, 2 * width), BF16),
            pltpu.VMEM(((LATENT + 1) * patches, width), BF16),
        ],
        compiler_params=pltpu.CompilerParams(vmem_limit_bytes=60 * 1024 * 1024),
    )(shift, state, normed, left, right, window_qkv, window_out)


def solution(mesh):
    in_specs = (P("tile", "member", None), P("tile", None), P("tile")) + (P(),) * 11
    out_specs = P(None, "tile", "member", None, None)
    return jax.shard_map(local, mesh=mesh, in_specs=in_specs, out_specs=out_specs, check_vma=False)
```

```python
import functools
import math

import jax
import jax.numpy as jnp
from jax import lax
from jax.experimental import pallas as pl
from jax.experimental.pallas import tpu as pltpu
from jax.sharding import PartitionSpec as P

LEVELS = 13
V_ATM = 5
V_SURF = 4
LATENT = 3
HEADS = 8
WL = 2
WH = 6
WW = 12
LT = 8
CHANNELS = V_ATM * LEVELS + V_SURF
F32 = jnp.float32
BF16 = jnp.bfloat16
NT = (((1,), (1,)), ((), ()))


def encode(
    n, cap, shift_ref, marked_ref, x_ref, weight, bias, code, latents, perc_query, perc_kv,
    perc_out, gain, qkv_ref, out_w_ref, out_ref, recv, emb, pair, logits, gath, recv_ids,
    inverse, ids, slot_of, bias_rows, code_rows, state_ref, normed_ref, left_ref, right_ref,
    own_triple, near_pair, mixed_ref, send_sem, recv_sem, table_send, table_recv, local_sem,
    rim_send, rim_recv,
):
    me = lax.axis_index("tile")
    bands = n // LT
    patches, packed = x_ref.shape[1:]
    pix = packed // cap
    width = weight.shape[2]
    head = width // HEADS

    barrier = pltpu.get_barrier_semaphore()

    def greet(k, carry):
        pl.semaphore_signal(barrier, inc=1, device_id={"tile": lax.rem(me + k, n)})
        return carry

    lax.fori_loop(1, n, greet, 0)
    pl.semaphore_wait(barrier, n - 1)

    def offset(i):
        half = n // 2
        step = (i + 1) // 2
        return half + step - 2 * step * (i % 2)

    def table_copy(k):
        return pltpu.make_async_remote_copy(
            src_ref=marked_ref,
            dst_ref=recv_ids.at[me],
            send_sem=table_send.at[k],
            recv_sem=table_recv.at[k],
            device_id={"tile": lax.rem(me + k, n)},
        )

    def copy(k):
        to = lax.rem(me + k, n)
        return pltpu.make_async_remote_copy(
            src_ref=x_ref.at[to],
            dst_ref=recv.at[me],
            send_sem=send_sem.at[k],
            recv_sem=recv_sem.at[k],
            device_id={"tile": to},
        )

    def launch(i, carry):
        table_copy(offset(i)).start()
        return carry

    lax.fori_loop(0, n - 1, launch, 0)

    def launch_block(i, carry):
        copy(offset(i)).start()
        return carry

    lax.fori_loop(0, n - 1, launch_block, 0)

    recv_ids[me] = marked_ref[...]
    for i in range(bias.shape[0]):
        bias_rows[i] = bias[i:i + 1, :].astype(F32)
    for i in range(code.shape[0]):
        code_rows[i] = code[i:i + 1, :].astype(F32)

    query = jnp.dot(latents[...], perc_query[...], preferred_element_type=F32) / math.sqrt(head)
    lane_head = lax.broadcasted_iota(jnp.int32, (HEADS, width), 1) // head
    row_head = lax.broadcasted_iota(jnp.int32, (HEADS, width), 0)
    own_head = lane_head == row_head
    spread = [jnp.where(own_head, query[j:j + 1, :], 0.0) for j in range(LATENT)]
    spread.append(jnp.zeros((HEADS, width), F32))
    rows = jnp.concatenate(spread, axis=0)
    rows_high = rows.astype(BF16)
    rows_low = (rows - rows_high.astype(F32)).astype(BF16)

    def table_land(k, carry):
        table_copy(k).wait_recv()
        return carry

    lax.fori_loop(1, n, table_land, 0)
    to_ids = pltpu.make_async_copy(recv_ids, ids, local_sem.at[0])
    to_ids.start()

    channel = lax.broadcasted_iota(jnp.int32, inverse.shape, 0)
    lane = lax.broadcasted_iota(jnp.int32, inverse.shape, 1)

    def match(d, found):
        hit = recv_ids[d] == channel
        return found + jnp.where(hit, (lane + d * cap).astype(F32), 0.0)

    found = lax.fori_loop(0, n, match, jnp.zeros(inverse.shape, F32))
    total = jnp.sum(found, axis=1, keepdims=True).astype(jnp.int32)
    inverse[...] = jnp.broadcast_to(total, inverse.shape)
    to_ids.wait()

    def embed(block, source):
        for s in range(cap):
            held = ids[source, 0, s]
            held = jnp.where(held >= CHANNELS, held - CHANNELS, held)
            kind = jnp.where(
                held < V_ATM * LEVELS, held // LEVELS, held - V_ATM * LEVELS + V_ATM
            )
            kind = jnp.clip(kind, 0, weight.shape[0] - 1)
            value = jnp.dot(
                block[:, s * pix:(s + 1) * pix], weight[kind], preferred_element_type=F32
            )
            emb[source * cap + s] = (value + bias_rows[kind]).astype(BF16)

    embed(x_ref[me], me)
    to_slots = pltpu.make_async_copy(inverse, slot_of, local_sem.at[1])
    to_slots.start()
    to_slots.wait()

    def land(i, carry):
        k = offset(i)
        copy(k).wait_recv()
        source = lax.rem(me + n - k, n)
        embed(recv[source], source)
        return carry

    lax.fori_loop(0, n - 1, land, 0)

    def channel_value(c):
        return emb[jnp.clip(slot_of[c, 0], 0, n * cap - 1)].astype(F32)

    def rim(j, side):
        to = lax.rem(me + bands, n) if side == 0 else lax.rem(me + n - bands, n)
        return pltpu.make_async_remote_copy(
            src_ref=normed_ref.at[j],
            dst_ref=(left_ref if side == 0 else right_ref).at[j],
            send_sem=rim_send.at[j, side],
            recv_sem=rim_recv.at[j, side],
            device_id={"tile": to},
        )

    def finish_level(j, state):
        center = state - jnp.mean(state, axis=-1, keepdims=True)
        spread_of = jnp.mean(center * center, axis=-1, keepdims=True)
        state_ref[j] = state
        normed_ref[j] = (
            center * lax.rsqrt(spread_of + 1e-05) * gain[...].astype(F32)
        ).astype(BF16)

    surface = channel_value(V_ATM * LEVELS)
    for c in range(V_ATM * LEVELS + 1, CHANNELS):
        surface = surface + channel_value(c)
    finish_level(LATENT, surface + code_rows[LEVELS])

    def one_level(l, carry):
        total = channel_value(l)
        for v in range(1, V_ATM):
            total = total + channel_value(v * LEVELS + l)
        token = (total + code_rows[l]).astype(BF16)
        both = jnp.dot(token, perc_kv[...], preferred_element_type=F32).astype(BF16)
        pair[l] = both[:, width:]
        keys = both[:, :width]
        logits[l] = lax.dot_general(
            keys, rows_high, NT, preferred_element_type=F32
        ) + lax.dot_general(keys, rows_low, NT, preferred_element_type=F32)
        return carry

    one_level(0, 0)
    for side in range(2):
        rim(LATENT, side).start()
    lax.fori_loop(1, LEVELS, one_level, 0)

    top = logits[0]
    for l in range(1, LEVELS):
        top = jnp.maximum(top, logits[l])
    norm = jnp.zeros_like(top)
    for l in range(LEVELS):
        power = jnp.exp(logits[l] - top)
        logits[l] = power
        norm = norm + power
    scale = 1.0 / norm

    wide_row = lax.broadcasted_iota(jnp.int32, (4 * HEADS, LATENT * width), 0)
    wide_lane = lax.broadcasted_iota(jnp.int32, (4 * HEADS, LATENT * width), 1) // head
    expand = jnp.where(wide_row == wide_lane, 1.0, 0.0).astype(BF16)
    gath[...] = jnp.zeros_like(gath)

    def weigh(l, carry):
        attn = (logits[l] * scale).astype(BF16)
        value = pair[l].astype(F32)
        wide = jnp.dot(attn, expand, preferred_element_type=F32)
        for j in range(LATENT):
            gath[j] += wide[:, j * width:(j + 1) * width] * value
        return carry

    lax.fori_loop(0, LEVELS, weigh, 0)

    def project_own(j):
        own_triple[j * patches:(j + 1) * patches, :] = jnp.dot(
            normed_ref[j], qkv_ref[...], preferred_element_type=F32
        ).astype(BF16)

    for j in range(LATENT):
        finish_level(j, latents[j:j + 1, :].astype(F32) + jnp.dot(
            gath[j].astype(BF16), perc_out[...], preferred_element_type=F32
        ))
        if j:
            for side in range(2):
                rim(j - 1, side).start()
    project_own(LATENT)
    for side in range(2):
        rim(LATENT - 1, side).start()
    for j in range(LATENT):
        project_own(j)

    first = shift_ref[0]
    column = lax.broadcasted_iota(jnp.int32, (patches, width), 0) % WW
    for j in (LATENT,) + tuple(range(LATENT)):
        for side in range(2):
            rim(j, side).wait_recv()
        near = jnp.where(
            column >= first, left_ref[j].astype(F32), right_ref[j].astype(F32)
        ).astype(BF16)
        near_pair[j * patches:(j + 1) * patches, :] = jnp.dot(
            near, qkv_ref[:, width:], preferred_element_type=F32
        ).astype(BF16)

    levels = LATENT + 1
    members = WL * patches
    q_first = lax.broadcasted_iota(jnp.int32, (members, members), 0) % WW < first
    k_first = lax.broadcasted_iota(jnp.int32, (members, members), 1) % WW < first
    same = q_first == k_first
    half_lane = lax.broadcasted_iota(jnp.int32, (members, 2 * head), 1) // head
    root = 1.0 / math.sqrt(head)
    for g in range(levels // WL):
        r = slice(g * members, (g + 1) * members)
        for h2 in range(HEADS // 2):
            c = slice(h2 * 2 * head, (h2 + 1) * 2 * head)
            ck = slice(width + h2 * 2 * head, width + (h2 + 1) * 2 * head)
            cv = slice(2 * width + h2 * 2 * head, 2 * width + (h2 + 1) * 2 * head)
            q = own_triple[r, c]
            k_own = own_triple[r, ck]
            v_own = own_triple[r, cv]
            k_near = near_pair[r, c]
            v_near = near_pair[r, ck]
            halves = []
            for one in range(2):
                q_one = jnp.where(half_lane == one, q, jnp.zeros_like(q))
                a = lax.dot_general(q_one, k_own, NT, preferred_element_type=F32) * root
                b = lax.dot_general(q_one, k_near, NT, preferred_element_type=F32) * root
                a = jnp.where(same, a, -jnp.inf)
                b = jnp.where(same, -jnp.inf, b)
                peak = jnp.maximum(
                    jnp.max(a, axis=-1, keepdims=True), jnp.max(b, axis=-1, keepdims=True)
                )
                a = jnp.exp(a - peak)
                b = jnp.exp(b - peak)
                unit = 1.0 / (
                    jnp.sum(a, axis=-1, keepdims=True) + jnp.sum(b, axis=-1, keepdims=True)
                )
                halves.append(
                    jnp.dot((a * unit).astype(BF16), v_own, preferred_element_type=F32)
                    + jnp.dot((b * unit).astype(BF16), v_near, preferred_element_type=F32)
                )
            mixed_ref[r, c] = jnp.where(half_lane == 0, halves[0], halves[1]).astype(BF16)
        result = jnp.dot(mixed_ref[r, :], out_w_ref[...], preferred_element_type=F32)
        for level in range(WL):
            j = g * WL + level
            full = state_ref[j] + result[level * patches:(level + 1) * patches, :]
            for i in range(WH):
                out_ref[j, 0, i] = full[i * WW:(i + 1) * WW, :].astype(BF16)

    def drain(k, carry):
        copy(k).wait_send()
        table_copy(k).wait_send()
        return carry

    lax.fori_loop(1, n, drain, 0)
    for j in range(levels):
        for side in range(2):
            rim(j, side).wait_send()


def local(
    pixels, channel_index_table, group_sizes, patch_weight, patch_bias, level_code, latents,
    perc_query, perc_kv, perc_out, norm_gain, window_qkv, window_out, shift,
):
    n = lax.axis_size("tile")
    cap, pix, all_patches = pixels.shape
    patches = all_patches // n
    kind_count, _, width = patch_weight.shape
    levels = LATENT + 1
    vmem = pl.BlockSpec(memory_space=pltpu.VMEM)
    smem = pl.BlockSpec(memory_space=pltpu.SMEM)

    slot = jnp.arange(cap, dtype=jnp.int32)[None, :]
    marked = jnp.where(
        slot < group_sizes[:, None], channel_index_table, channel_index_table + CHANNELS
    )
    marked = jnp.pad(marked, ((0, 0), (0, 128 - cap)), constant_values=-1)
    blocks = pixels.reshape(cap * pix, all_patches).T.reshape(n, patches, cap * pix)
    inverse_shape = (-(-CHANNELS // 8) * 8, 128)
    return pl.pallas_call(
        functools.partial(encode, n, cap),
        out_shape=jax.ShapeDtypeStruct((levels, 1, WH, patches // WH, width), BF16),
        in_specs=[smem] + [vmem] * 12,
        out_specs=vmem,
        scratch_shapes=[
            pltpu.VMEM((n, patches, cap * pix), BF16),
            pltpu.VMEM((n * cap, patches, width), BF16),
            pltpu.VMEM((LEVELS, patches, width), BF16),
            pltpu.VMEM((LEVELS, patches, 4 * HEADS), F32),
            pltpu.VMEM((LATENT, patches, width), F32),
            pltpu.VMEM((n, 1, 128), jnp.int32),
            pltpu.VMEM(inverse_shape, jnp.int32),
            pltpu.SMEM((n, 1, 128), jnp.int32),
            pltpu.SMEM(inverse_shape, jnp.int32),
            pltpu.VMEM((kind_count, 1, width), F32),
            pltpu.VMEM((LEVELS + 1, 1, width), F32),
            pltpu.VMEM((levels, patches, width), F32),
            pltpu.VMEM((levels, patches, width), BF16),
            pltpu.VMEM((levels, patches, width), BF16),
            pltpu.VMEM((levels, patches, width), BF16),
            pltpu.VMEM((levels * patches, 3 * width), BF16),
            pltpu.VMEM((levels * patches, 2 * width), BF16),
            pltpu.VMEM((levels * patches, width), BF16),
            pltpu.SemaphoreType.DMA((n,)),
            pltpu.SemaphoreType.DMA((n,)),
            pltpu.SemaphoreType.DMA((n,)),
            pltpu.SemaphoreType.DMA((n,)),
            pltpu.SemaphoreType.DMA((2,)),
            pltpu.SemaphoreType.DMA((levels, 2)),
            pltpu.SemaphoreType.DMA((levels, 2)),
        ],
        compiler_params=pltpu.CompilerParams(
            collective_id=0, has_side_effects=True, vmem_limit_bytes=60 * 1024 * 1024
        ),
    )(
        shift, marked, blocks, patch_weight, patch_bias, level_code, latents, perc_query,
        perc_kv, perc_out, norm_gain.reshape(1, width), window_qkv, window_out,
    )


def solution(mesh):
    in_specs = (P("tile", "member", None), P("tile", None), P("tile")) + (P(),) * 11
    out_specs = P(None, "tile", "member", None, None)
    return jax.shard_map(local, mesh=mesh, in_specs=in_specs, out_specs=out_specs, check_vma=False)
```

```python
import functools
import math

import jax
import jax.numpy as jnp
from jax import lax
from jax.experimental import pallas as pl
from jax.experimental.pallas import tpu as pltpu
from jax.sharding import PartitionSpec as P

LEVELS = 13
V_ATM = 5
V_SURF = 4
LATENT = 3
HEADS = 8
WL = 2
WH = 6
WW = 12
LT = 8
CHANNELS = V_ATM * LEVELS + V_SURF
F32 = jnp.float32
BF16 = jnp.bfloat16
NT = (((1,), (1,)), ((), ()))


def encode(
    n, cap, shift_ref, sizes_ref, table_ref, bias, code, latents, gain, x_ref, *refs
):
    hbm_weights, (out_ref, marked_ref), refs = refs[:6], refs[6:8], refs[8:]
    vmem_weights, refs = refs[:6], refs[6:]
    weight, perc_query, perc_kv, perc_out, qkv_ref, out_w_ref = vmem_weights
    (
    recv, emb, pair, logits, recv_ids,
    inverse, ids, slot_of, bias_rows, code_rows, state_ref, normed_ref, left_ref, right_ref,
    own_triple, near_pair, mixed_ref, send_sem, recv_sem, table_send, table_recv, local_sem,
    rim_send, rim_recv, weight_sem,
    ) = refs
    me = lax.axis_index("tile")
    bands = n // LT
    patches, packed = x_ref.shape[1:]
    pix = packed // cap
    width = weight.shape[2]
    head = width // HEADS

    barrier = pltpu.get_barrier_semaphore()

    def greet(k, carry):
        pl.semaphore_signal(barrier, inc=1, device_id={"tile": lax.rem(me + k, n)})
        return carry

    lax.fori_loop(1, n, greet, 0)
    fetches = [
        pltpu.make_async_copy(source, target, weight_sem.at[i])
        for i, (source, target) in enumerate(zip(hbm_weights, vmem_weights))
    ]
    for fetch in fetches[:2]:
        fetch.start()
    own_block = pltpu.make_async_copy(x_ref.at[me], recv.at[me], local_sem.at[2])
    own_block.start()
    lane = lax.broadcasted_iota(jnp.int32, (1, cap), 1)
    table = table_ref[...]
    marked_ref[...] = jnp.full(marked_ref.shape, -1, jnp.int32)
    marked_ref[:, :cap] = jnp.where(lane < sizes_ref[0], table, table + CHANNELS)
    pl.semaphore_wait(barrier, n - 1)

    def offset(i):
        half = n // 2
        step = (i + 1) // 2
        return half + step - 2 * step * (i % 2)

    def table_copy(k):
        return pltpu.make_async_remote_copy(
            src_ref=marked_ref,
            dst_ref=recv_ids.at[me],
            send_sem=table_send.at[k],
            recv_sem=table_recv.at[k],
            device_id={"tile": lax.rem(me + k, n)},
        )

    def copy(k):
        to = lax.rem(me + k, n)
        return pltpu.make_async_remote_copy(
            src_ref=x_ref.at[to],
            dst_ref=recv.at[me],
            send_sem=send_sem.at[k],
            recv_sem=recv_sem.at[k],
            device_id={"tile": to},
        )

    def launch(i, carry):
        table_copy(offset(i)).start()
        return carry

    lax.fori_loop(0, n - 1, launch, 0)

    def launch_block(i, carry):
        copy(offset(i)).start()
        return carry

    lax.fori_loop(0, n - 1, launch_block, 0)

    for fetch in fetches[2:]:
        fetch.start()
    recv_ids[me] = marked_ref[...]
    for i in range(bias.shape[0]):
        bias_rows[i] = bias[i:i + 1, :].astype(F32)
    for i in range(code.shape[0]):
        code_rows[i] = code[i:i + 1, :].astype(F32)

    fetches[1].wait()
    query = jnp.dot(latents[...], perc_query[...], preferred_element_type=F32) / math.sqrt(head)
    lane_head = lax.broadcasted_iota(jnp.int32, (HEADS, width), 1) // head
    row_head = lax.broadcasted_iota(jnp.int32, (HEADS, width), 0)
    own_head = lane_head == row_head
    spread = [jnp.where(own_head, query[j:j + 1, :], 0.0) for j in range(LATENT)]
    spread.append(jnp.zeros((HEADS, width), F32))
    rows = jnp.concatenate(spread, axis=0)
    rows_high = rows.astype(BF16)
    rows_low = (rows - rows_high.astype(F32)).astype(BF16)

    def table_land(k, carry):
        table_copy(k).wait_recv()
        return carry

    lax.fori_loop(1, n, table_land, 0)
    to_ids = pltpu.make_async_copy(recv_ids, ids, local_sem.at[0])
    to_ids.start()

    channel = lax.broadcasted_iota(jnp.int32, inverse.shape, 0)
    lane = lax.broadcasted_iota(jnp.int32, inverse.shape, 1)

    def match(d, found):
        hit = recv_ids[d] == channel
        return found + jnp.where(hit, (lane + d * cap).astype(F32), 0.0)

    found = lax.fori_loop(0, n, match, jnp.zeros(inverse.shape, F32))
    total = jnp.sum(found, axis=1, keepdims=True).astype(jnp.int32)
    inverse[...] = jnp.broadcast_to(total, inverse.shape)
    to_ids.wait()

    def embed(block, source):
        for s in range(cap):
            held = ids[source, 0, s]
            held = jnp.where(held >= CHANNELS, held - CHANNELS, held)
            kind = jnp.where(
                held < V_ATM * LEVELS, held // LEVELS, held - V_ATM * LEVELS + V_ATM
            )
            kind = jnp.clip(kind, 0, weight.shape[0] - 1)
            value = jnp.dot(
                block[:, s * pix:(s + 1) * pix], weight[kind], preferred_element_type=F32
            )
            emb[source * cap + s] = (value + bias_rows[kind]).astype(BF16)

    fetches[0].wait()
    own_block.wait()
    embed(recv[me], me)
    to_slots = pltpu.make_async_copy(inverse, slot_of, local_sem.at[1])
    to_slots.start()
    to_slots.wait()

    def land(i, carry):
        k = offset(i)
        copy(k).wait_recv()
        source = lax.rem(me + n - k, n)
        embed(recv[source], source)
        return carry

    for fetch in fetches[2:]:
        fetch.wait()
    lax.fori_loop(0, n - 1, land, 0)

    def channel_value(c):
        return emb[jnp.clip(slot_of[c, 0], 0, n * cap - 1)].astype(F32)

    def rim(j, side):
        to = lax.rem(me + bands, n) if side == 0 else lax.rem(me + n - bands, n)
        return pltpu.make_async_remote_copy(
            src_ref=normed_ref.at[j],
            dst_ref=(left_ref if side == 0 else right_ref).at[j],
            send_sem=rim_send.at[j, side],
            recv_sem=rim_recv.at[j, side],
            device_id={"tile": to},
        )

    gain_row = gain[...].astype(F32).reshape(1, width)

    def finish_level(j, state):
        center = state - jnp.mean(state, axis=-1, keepdims=True)
        spread_of = jnp.mean(center * center, axis=-1, keepdims=True)
        state_ref[j] = state
        normed_ref[j] = (
            center * lax.rsqrt(spread_of + 1e-05) * gain_row
        ).astype(BF16)

    surface = channel_value(V_ATM * LEVELS)
    for c in range(V_ATM * LEVELS + 1, CHANNELS):
        surface = surface + channel_value(c)
    finish_level(LATENT, surface + code_rows[LEVELS])

    def one_level(l, carry):
        total = channel_value(l)
        for v in range(1, V_ATM):
            total = total + channel_value(v * LEVELS + l)
        token = (total + code_rows[l]).astype(BF16)
        both = jnp.dot(token, perc_kv[...], preferred_element_type=F32).astype(BF16)
        pair[l] = both[:, width:]
        keys = both[:, :width]
        logits[l] = lax.dot_general(
            keys, rows_high, NT, preferred_element_type=F32
        ) + lax.dot_general(keys, rows_low, NT, preferred_element_type=F32)
        return carry

    one_level(0, 0)
    for side in range(2):
        rim(LATENT, side).start()
    lax.fori_loop(1, LEVELS, one_level, 0)

    top = logits[0]
    for l in range(1, LEVELS):
        top = jnp.maximum(top, logits[l])
    norm = jnp.zeros_like(top)
    for l in range(LEVELS):
        power = jnp.exp(logits[l] - top)
        logits[l] = power
        norm = norm + power
    scale = 1.0 / norm

    wide_row = lax.broadcasted_iota(jnp.int32, (4 * HEADS, width), 0)
    wide_lane = lax.broadcasted_iota(jnp.int32, (4 * HEADS, width), 1) // head

    def project_own(j):
        own_triple[j * patches:(j + 1) * patches, :] = jnp.dot(
            normed_ref[j], qkv_ref[...], preferred_element_type=F32
        ).astype(BF16)

    first = shift_ref[0]
    column = lax.broadcasted_iota(jnp.int32, (patches, width), 0) % WW

    def project_near(j):
        for side in range(2):
            rim(j, side).wait_recv()
        near = jnp.where(
            column >= first, left_ref[j].astype(F32), right_ref[j].astype(F32)
        ).astype(BF16)
        near_pair[j * patches:(j + 1) * patches, :] = jnp.dot(
            near, qkv_ref[:, width:], preferred_element_type=F32
        ).astype(BF16)

    for l in range(LEVELS):
        logits[l] = (logits[l] * scale).astype(BF16).astype(F32)
    for j in range(LATENT):
        expand = jnp.where(wide_row == wide_lane + j * HEADS, 1.0, 0.0).astype(BF16)
        gathered = jnp.zeros((patches, width), F32)
        for l in range(LEVELS):
            wide = jnp.dot(logits[l].astype(BF16), expand, preferred_element_type=F32)
            gathered = gathered + wide * pair[l].astype(F32)
        finish_level(j, latents[j:j + 1, :].astype(F32) + jnp.dot(
            gathered.astype(BF16), perc_out[...], preferred_element_type=F32
        ))
        project_own(j)
        for side in range(2):
            rim(j, side).start()
    project_own(LATENT)

    levels = LATENT + 1
    members = WL * patches
    q_first = lax.broadcasted_iota(jnp.int32, (members, members), 0) % WW < first
    k_first = lax.broadcasted_iota(jnp.int32, (members, members), 1) % WW < first
    same = q_first == k_first
    half_lane = lax.broadcasted_iota(jnp.int32, (members, 2 * head), 1) // head
    root = 1.0 / math.sqrt(head)
    for g in range(levels // WL):
        for level in reversed(range(WL)):
            project_near(g * WL + level)
        r = slice(g * members, (g + 1) * members)
        for h2 in range(HEADS // 2):
            c = slice(h2 * 2 * head, (h2 + 1) * 2 * head)
            ck = slice(width + h2 * 2 * head, width + (h2 + 1) * 2 * head)
            cv = slice(2 * width + h2 * 2 * head, 2 * width + (h2 + 1) * 2 * head)
            q = own_triple[r, c]
            k_own = own_triple[r, ck]
            v_own = own_triple[r, cv]
            k_near = near_pair[r, c]
            v_near = near_pair[r, ck]
            halves = []
            for one in range(2):
                q_one = jnp.where(half_lane == one, q, jnp.zeros_like(q))
                a = lax.dot_general(q_one, k_own, NT, preferred_element_type=F32) * root
                b = lax.dot_general(q_one, k_near, NT, preferred_element_type=F32) * root
                both = jnp.where(same, a, b)
                both = jnp.exp(both - jnp.max(both, axis=-1, keepdims=True))
                both = both * (1.0 / jnp.sum(both, axis=-1, keepdims=True))
                halves.append(
                    jnp.dot(
                        jnp.where(same, both, 0.0).astype(BF16), v_own,
                        preferred_element_type=F32,
                    )
                    + jnp.dot(
                        jnp.where(same, 0.0, both).astype(BF16), v_near,
                        preferred_element_type=F32,
                    )
                )
            mixed_ref[r, c] = jnp.where(half_lane == 0, halves[0], halves[1]).astype(BF16)
        result = jnp.dot(mixed_ref[r, :], out_w_ref[...], preferred_element_type=F32)
        for level in range(WL):
            j = g * WL + level
            full = state_ref[j] + result[level * patches:(level + 1) * patches, :]
            for i in range(WH):
                out_ref[j, 0, i] = full[i * WW:(i + 1) * WW, :].astype(BF16)

    def drain(k, carry):
        copy(k).wait_send()
        table_copy(k).wait_send()
        return carry

    lax.fori_loop(1, n, drain, 0)
    for j in range(levels):
        for side in range(2):
            rim(j, side).wait_send()


def local(
    pixels, channel_index_table, group_sizes, patch_weight, patch_bias, level_code, latents,
    perc_query, perc_kv, perc_out, norm_gain, window_qkv, window_out, shift,
):
    n = lax.axis_size("tile")
    cap, pix, all_patches = pixels.shape
    patches = all_patches // n
    kind_count, _, width = patch_weight.shape
    levels = LATENT + 1
    vmem = pl.BlockSpec(memory_space=pltpu.VMEM)
    smem = pl.BlockSpec(memory_space=pltpu.SMEM)
    stays = pl.BlockSpec(memory_space=pl.ANY)
    weights = (patch_weight, perc_query, perc_kv, perc_out, window_qkv, window_out)

    blocks = pixels.reshape(cap * pix, all_patches).T.reshape(n, patches, cap * pix)
    inverse_shape = (-(-CHANNELS // 8) * 8, 128)
    return pl.pallas_call(
        functools.partial(encode, n, cap),
        out_shape=jax.ShapeDtypeStruct((levels, 1, WH, patches // WH, width), BF16),
        in_specs=[smem] * 2 + [vmem] * 5 + [stays] * 7,
        out_specs=vmem,
        scratch_shapes=[
            pltpu.VMEM((1, 128), jnp.int32),
            *[pltpu.VMEM(w.shape, BF16) for w in weights],
            pltpu.VMEM((n, patches, cap * pix), BF16),
            pltpu.VMEM((n * cap, patches, width), BF16),
            pltpu.VMEM((LEVELS, patches, width), BF16),
            pltpu.VMEM((LEVELS, patches, 4 * HEADS), F32),
            pltpu.VMEM((n, 1, 128), jnp.int32),
            pltpu.VMEM(inverse_shape, jnp.int32),
            pltpu.SMEM((n, 1, 128), jnp.int32),
            pltpu.SMEM(inverse_shape, jnp.int32),
            pltpu.VMEM((kind_count, 1, width), F32),
            pltpu.VMEM((LEVELS + 1, 1, width), F32),
            pltpu.VMEM((levels, patches, width), F32),
            pltpu.VMEM((levels, patches, width), BF16),
            pltpu.VMEM((levels, patches, width), BF16),
            pltpu.VMEM((levels, patches, width), BF16),
            pltpu.VMEM((levels * patches, 3 * width), BF16),
            pltpu.VMEM((levels * patches, 2 * width), BF16),
            pltpu.VMEM((levels * patches, width), BF16),
            pltpu.SemaphoreType.DMA((n,)),
            pltpu.SemaphoreType.DMA((n,)),
            pltpu.SemaphoreType.DMA((n,)),
            pltpu.SemaphoreType.DMA((n,)),
            pltpu.SemaphoreType.DMA((3,)),
            pltpu.SemaphoreType.DMA((levels, 2)),
            pltpu.SemaphoreType.DMA((levels, 2)),
            pltpu.SemaphoreType.DMA((len(weights),)),
        ],
        compiler_params=pltpu.CompilerParams(
            collective_id=0, has_side_effects=True, vmem_limit_bytes=60 * 1024 * 1024
        ),
    )(
        shift, group_sizes, channel_index_table, patch_bias, level_code, latents, norm_gain,
        blocks, *weights,
    )


def solution(mesh):
    in_specs = (P("tile", "member", None), P("tile", None), P("tile")) + (P(),) * 11
    out_specs = P(None, "tile", "member", None, None)
    return jax.shard_map(local, mesh=mesh, in_specs=in_specs, out_specs=out_specs, check_vma=False)
```

```python
import functools
import math

import jax
import jax.numpy as jnp
from jax import lax
from jax.experimental import pallas as pl
from jax.experimental.pallas import tpu as pltpu
from jax.sharding import PartitionSpec as P

LEVELS = 13
V_ATM = 5
V_SURF = 4
LATENT = 3
HEADS = 8
WL = 2
WH = 6
WW = 12
LT = 8
CHANNELS = V_ATM * LEVELS + V_SURF
F32 = jnp.float32
BF16 = jnp.bfloat16
NT = (((1,), (1,)), ((), ()))


def encode(
    n, cap, shift_ref, sizes_ref, table_ref, bias, code, latents, gain, x_ref, *refs
):
    hbm_weights, (out_ref, marked_ref), refs = refs[:6], refs[6:8], refs[8:]
    vmem_weights, refs = refs[:6], refs[6:]
    weight, perc_query, perc_kv, perc_out, qkv_ref, out_w_ref = vmem_weights
    (
    recv, emb, pair, logits, recv_ids,
    inverse, ids, slot_of, bias_rows, code_rows, state_ref, normed_ref, left_ref, right_ref,
    own_triple, near_pair, mixed_ref, send_sem, recv_sem, table_send, table_recv, local_sem,
    rim_send, rim_recv, weight_sem, tokens,
    ) = refs
    me = lax.axis_index("tile")
    bands = n // LT
    patches, packed = x_ref.shape[1:]
    pix = packed // cap
    width = weight.shape[2]
    head = width // HEADS

    barrier = pltpu.get_barrier_semaphore()

    def greet(k, carry):
        pl.semaphore_signal(barrier, inc=1, device_id={"tile": lax.rem(me + k, n)})
        return carry

    lax.fori_loop(1, n, greet, 0)
    fetches = [
        pltpu.make_async_copy(source, target, weight_sem.at[i])
        for i, (source, target) in enumerate(zip(hbm_weights, vmem_weights))
    ]
    for fetch in fetches[:2]:
        fetch.start()
    own_block = pltpu.make_async_copy(x_ref.at[me], recv.at[me], local_sem.at[2])
    own_block.start()
    lane = lax.broadcasted_iota(jnp.int32, (1, cap), 1)
    table = table_ref[...]
    marked_ref[...] = jnp.full(marked_ref.shape, -1, jnp.int32)
    marked_ref[:, :cap] = jnp.where(lane < sizes_ref[0], table, table + CHANNELS)
    pl.semaphore_wait(barrier, n - 1)

    def offset(i):
        half = n // 2
        step = (i + 1) // 2
        return half + step - 2 * step * (i % 2)

    def table_copy(k):
        return pltpu.make_async_remote_copy(
            src_ref=marked_ref,
            dst_ref=recv_ids.at[me],
            send_sem=table_send.at[k],
            recv_sem=table_recv.at[k],
            device_id={"tile": lax.rem(me + k, n)},
        )

    def copy(k):
        to = lax.rem(me + k, n)
        return pltpu.make_async_remote_copy(
            src_ref=x_ref.at[to],
            dst_ref=recv.at[me],
            send_sem=send_sem.at[k],
            recv_sem=recv_sem.at[k],
            device_id={"tile": to},
        )

    def launch(i, carry):
        table_copy(offset(i)).start()
        return carry

    lax.fori_loop(0, n - 1, launch, 0)

    def launch_block(i, carry):
        copy(offset(i)).start()
        return carry

    lax.fori_loop(0, n - 1, launch_block, 0)

    for fetch in fetches[2:]:
        fetch.start()
    recv_ids[me] = marked_ref[...]
    for i in range(bias.shape[0]):
        bias_rows[i] = bias[i:i + 1, :].astype(F32)
    for i in range(code.shape[0]):
        code_rows[i] = code[i:i + 1, :].astype(F32)

    fetches[1].wait()
    query = jnp.dot(latents[...], perc_query[...], preferred_element_type=F32) / math.sqrt(head)
    lane_head = lax.broadcasted_iota(jnp.int32, (HEADS, width), 1) // head
    row_head = lax.broadcasted_iota(jnp.int32, (HEADS, width), 0)
    own_head = lane_head == row_head
    spread = [jnp.where(own_head, query[j:j + 1, :], 0.0) for j in range(LATENT)]
    spread.append(jnp.zeros((HEADS, width), F32))
    rows = jnp.concatenate(spread, axis=0)
    rows_high = rows.astype(BF16)
    rows_low = (rows - rows_high.astype(F32)).astype(BF16)

    def table_land(k, carry):
        table_copy(k).wait_recv()
        return carry

    lax.fori_loop(1, n, table_land, 0)
    to_ids = pltpu.make_async_copy(recv_ids, ids, local_sem.at[0])
    to_ids.start()

    channel = lax.broadcasted_iota(jnp.int32, inverse.shape, 0)
    lane = lax.broadcasted_iota(jnp.int32, inverse.shape, 1)

    def match(d, found):
        hit = recv_ids[d] == channel
        return found + jnp.where(hit, (lane + d * cap).astype(F32), 0.0)

    found = lax.fori_loop(0, n, match, jnp.zeros(inverse.shape, F32))
    total = jnp.sum(found, axis=1, keepdims=True).astype(jnp.int32)
    inverse[...] = jnp.broadcast_to(total, inverse.shape)
    to_ids.wait()

    def embed(block, source):
        for s in range(cap):
            held = ids[source, 0, s]
            held = jnp.where(held >= CHANNELS, held - CHANNELS, held)
            kind = jnp.where(
                held < V_ATM * LEVELS, held // LEVELS, held - V_ATM * LEVELS + V_ATM
            )
            kind = jnp.clip(kind, 0, weight.shape[0] - 1)
            value = jnp.dot(
                block[:, s * pix:(s + 1) * pix], weight[kind], preferred_element_type=F32
            )
            emb[source * cap + s] = (value + bias_rows[kind]).astype(BF16)

    fetches[0].wait()
    own_block.wait()
    embed(recv[me], me)
    to_slots = pltpu.make_async_copy(inverse, slot_of, local_sem.at[1])
    to_slots.start()
    to_slots.wait()

    def land(i, carry):
        k = offset(i)
        copy(k).wait_recv()
        source = lax.rem(me + n - k, n)
        embed(recv[source], source)
        return carry

    for fetch in fetches[2:]:
        fetch.wait()
    lax.fori_loop(0, n - 1, land, 0)

    def channel_value(c):
        return emb[jnp.clip(slot_of[c, 0], 0, n * cap - 1)].astype(F32)

    def rim(j, side):
        to = lax.rem(me + bands, n) if side == 0 else lax.rem(me + n - bands, n)
        return pltpu.make_async_remote_copy(
            src_ref=normed_ref.at[j],
            dst_ref=(left_ref if side == 0 else right_ref).at[j],
            send_sem=rim_send.at[j, side],
            recv_sem=rim_recv.at[j, side],
            device_id={"tile": to},
        )

    gain_row = gain[...].astype(F32).reshape(1, width)

    def finish_level(j, state):
        center = state - jnp.mean(state, axis=-1, keepdims=True)
        spread_of = jnp.mean(center * center, axis=-1, keepdims=True)
        state_ref[j] = state
        normed_ref[j] = (
            center * lax.rsqrt(spread_of + 1e-05) * gain_row
        ).astype(BF16)

    surface = channel_value(V_ATM * LEVELS)
    for c in range(V_ATM * LEVELS + 1, CHANNELS):
        surface = surface + channel_value(c)
    finish_level(LATENT, surface + code_rows[LEVELS])

    for l in range(LEVELS):
        total = channel_value(l)
        for v in range(1, V_ATM):
            total = total + channel_value(v * LEVELS + l)
        tokens[l * patches:(l + 1) * patches, :] = (total + code_rows[l]).astype(BF16)
    for side in range(2):
        rim(LATENT, side).start()
    keys = jnp.dot(tokens[...], perc_kv[:, :width], preferred_element_type=F32).astype(BF16)
    scores = lax.dot_general(
        keys, rows_high, NT, preferred_element_type=F32
    ) + lax.dot_general(keys, rows_low, NT, preferred_element_type=F32)
    values = jnp.dot(tokens[...], perc_kv[:, width:], preferred_element_type=F32).astype(BF16)
    for l in range(LEVELS):
        logits[l] = scores[l * patches:(l + 1) * patches, :]
        pair[l] = values[l * patches:(l + 1) * patches, :]

    top = logits[0]
    for l in range(1, LEVELS):
        top = jnp.maximum(top, logits[l])
    norm = jnp.zeros_like(top)
    for l in range(LEVELS):
        power = jnp.exp(logits[l] - top)
        logits[l] = power
        norm = norm + power
    scale = 1.0 / norm

    wide_row = lax.broadcasted_iota(jnp.int32, (4 * HEADS, width), 0)
    wide_lane = lax.broadcasted_iota(jnp.int32, (4 * HEADS, width), 1) // head

    def project_own(j):
        own_triple[j * patches:(j + 1) * patches, :] = jnp.dot(
            normed_ref[j], qkv_ref[...], preferred_element_type=F32
        ).astype(BF16)

    first = shift_ref[0]
    column = lax.broadcasted_iota(jnp.int32, (patches, width), 0) % WW

    def project_near(j):
        for side in range(2):
            rim(j, side).wait_recv()
        near = jnp.where(
            column >= first, left_ref[j].astype(F32), right_ref[j].astype(F32)
        ).astype(BF16)
        near_pair[j * patches:(j + 1) * patches, :] = jnp.dot(
            near, qkv_ref[:, width:], preferred_element_type=F32
        ).astype(BF16)

    for l in range(LEVELS):
        logits[l] = (logits[l] * scale).astype(BF16).astype(F32)
    for j in range(LATENT):
        expand = jnp.where(wide_row == wide_lane + j * HEADS, 1.0, 0.0).astype(BF16)
        gathered = jnp.zeros((patches, width), F32)
        for l in range(LEVELS):
            wide = jnp.dot(logits[l].astype(BF16), expand, preferred_element_type=F32)
            gathered = gathered + wide * pair[l].astype(F32)
        finish_level(j, latents[j:j + 1, :].astype(F32) + jnp.dot(
            gathered.astype(BF16), perc_out[...], preferred_element_type=F32
        ))
        project_own(j)
        for side in range(2):
            rim(j, side).start()
    project_own(LATENT)

    levels = LATENT + 1
    members = WL * patches
    q_first = lax.broadcasted_iota(jnp.int32, (members, members), 0) % WW < first
    k_first = lax.broadcasted_iota(jnp.int32, (members, members), 1) % WW < first
    same = q_first == k_first
    half_lane = lax.broadcasted_iota(jnp.int32, (members, 2 * head), 1) // head
    root = 1.0 / math.sqrt(head)
    for g in range(levels // WL):
        for level in reversed(range(WL)):
            project_near(g * WL + level)
        r = slice(g * members, (g + 1) * members)
        for h2 in range(HEADS // 2):
            c = slice(h2 * 2 * head, (h2 + 1) * 2 * head)
            ck = slice(width + h2 * 2 * head, width + (h2 + 1) * 2 * head)
            cv = slice(2 * width + h2 * 2 * head, 2 * width + (h2 + 1) * 2 * head)
            q = own_triple[r, c]
            k_own = own_triple[r, ck]
            v_own = own_triple[r, cv]
            k_near = near_pair[r, c]
            v_near = near_pair[r, ck]
            halves = []
            for one in range(2):
                q_one = jnp.where(half_lane == one, q, jnp.zeros_like(q))
                a = lax.dot_general(q_one, k_own, NT, preferred_element_type=F32) * root
                b = lax.dot_general(q_one, k_near, NT, preferred_element_type=F32) * root
                both = jnp.where(same, a, b)
                both = jnp.exp(both - jnp.max(both, axis=-1, keepdims=True))
                both = both * (1.0 / jnp.sum(both, axis=-1, keepdims=True))
                halves.append(
                    jnp.dot(
                        jnp.where(same, both, 0.0).astype(BF16), v_own,
                        preferred_element_type=F32,
                    )
                    + jnp.dot(
                        jnp.where(same, 0.0, both).astype(BF16), v_near,
                        preferred_element_type=F32,
                    )
                )
            mixed_ref[r, c] = jnp.where(half_lane == 0, halves[0], halves[1]).astype(BF16)
        result = jnp.dot(mixed_ref[r, :], out_w_ref[...], preferred_element_type=F32)
        for level in range(WL):
            j = g * WL + level
            full = state_ref[j] + result[level * patches:(level + 1) * patches, :]
            for i in range(WH):
                out_ref[j, 0, i] = full[i * WW:(i + 1) * WW, :].astype(BF16)

    def drain(k, carry):
        copy(k).wait_send()
        table_copy(k).wait_send()
        return carry

    lax.fori_loop(1, n, drain, 0)
    for j in range(levels):
        for side in range(2):
            rim(j, side).wait_send()


def local(
    pixels, channel_index_table, group_sizes, patch_weight, patch_bias, level_code, latents,
    perc_query, perc_kv, perc_out, norm_gain, window_qkv, window_out, shift,
):
    n = lax.axis_size("tile")
    cap, pix, all_patches = pixels.shape
    patches = all_patches // n
    kind_count, _, width = patch_weight.shape
    levels = LATENT + 1
    vmem = pl.BlockSpec(memory_space=pltpu.VMEM)
    smem = pl.BlockSpec(memory_space=pltpu.SMEM)
    stays = pl.BlockSpec(memory_space=pl.ANY)
    weights = (patch_weight, perc_query, perc_kv, perc_out, window_qkv, window_out)

    blocks = pixels.reshape(cap * pix, all_patches).T.reshape(n, patches, cap * pix)
    inverse_shape = (-(-CHANNELS // 8) * 8, 128)
    return pl.pallas_call(
        functools.partial(encode, n, cap),
        out_shape=jax.ShapeDtypeStruct((levels, 1, WH, patches // WH, width), BF16),
        in_specs=[smem] * 2 + [vmem] * 5 + [stays] * 7,
        out_specs=vmem,
        scratch_shapes=[
            pltpu.VMEM((1, 128), jnp.int32),
            *[pltpu.VMEM(w.shape, BF16) for w in weights],
            pltpu.VMEM((n, patches, cap * pix), BF16),
            pltpu.VMEM((n * cap, patches, width), BF16),
            pltpu.VMEM((LEVELS, patches, width), BF16),
            pltpu.VMEM((LEVELS, patches, 4 * HEADS), F32),
            pltpu.VMEM((n, 1, 128), jnp.int32),
            pltpu.VMEM(inverse_shape, jnp.int32),
            pltpu.SMEM((n, 1, 128), jnp.int32),
            pltpu.SMEM(inverse_shape, jnp.int32),
            pltpu.VMEM((kind_count, 1, width), F32),
            pltpu.VMEM((LEVELS + 1, 1, width), F32),
            pltpu.VMEM((levels, patches, width), F32),
            pltpu.VMEM((levels, patches, width), BF16),
            pltpu.VMEM((levels, patches, width), BF16),
            pltpu.VMEM((levels, patches, width), BF16),
            pltpu.VMEM((levels * patches, 3 * width), BF16),
            pltpu.VMEM((levels * patches, 2 * width), BF16),
            pltpu.VMEM((levels * patches, width), BF16),
            pltpu.SemaphoreType.DMA((n,)),
            pltpu.SemaphoreType.DMA((n,)),
            pltpu.SemaphoreType.DMA((n,)),
            pltpu.SemaphoreType.DMA((n,)),
            pltpu.SemaphoreType.DMA((3,)),
            pltpu.SemaphoreType.DMA((levels, 2)),
            pltpu.SemaphoreType.DMA((levels, 2)),
            pltpu.SemaphoreType.DMA((len(weights),)),
            pltpu.VMEM((LEVELS * patches, width), BF16),
        ],
        compiler_params=pltpu.CompilerParams(
            collective_id=0, has_side_effects=True, vmem_limit_bytes=60 * 1024 * 1024
        ),
    )(
        shift, group_sizes, channel_index_table, patch_bias, level_code, latents, norm_gain,
        blocks, *weights,
    )


def solution(mesh):
    in_specs = (P("tile", "member", None), P("tile", None), P("tile")) + (P(),) * 11
    out_specs = P(None, "tile", "member", None, None)
    return jax.shard_map(local, mesh=mesh, in_specs=in_specs, out_specs=out_specs, check_vma=False)
```
